16 devices in a mesh: dp: 2 (over y, z), tp: 8 (over x, core).
Axes of the slice: x: 4, y: 2, z: 1, core: 2. Of those that a mesh axis runs over, the one named last changes fastest.
The devices are a block of a 4x4x8 slice.
Arguments:
- tok_ids: int32 [1024], P('dp'), parts along dimension 0
- emb_table: bfloat16 [151936, 896], P('tp')
- norm_gain: bfloat16 [896], replicated
- w_in: bfloat16 [896, 4864], P(None, 'tp')
- w_out: bfloat16 [4864, 896], P('tp')
- d_out: bfloat16 [1024, 896], P(('dp', 'tp')), parts along dimension 0
Outputs:
- output 1: bfloat16 [1024, 896], P(('dp', 'tp')), parts along dimension 0
- output 2: float32 [303872, 896], P(('dp', 'tp')), parts along dimension 0
- output 3: float32 [1792, 4864], P('dp', 'tp'), parts along dimension 0
- output 4: float32 [9728, 896], P(('dp', 'tp')), parts along dimension 0
There are 2 independent parts. The reference program is written for one: setup_inputs(seed, part) draws one part's arguments, and reference() takes and returns one part's arrays. A program takes and returns all parts, laid end to end along the dimension named above; an argument that names none is the same for every part.
All inputs are finite; a program needn't handle non-finite values.
Results may differ from the reference program's by a relative error of at most 0.00580482.
Values are sent between devices in bfloat16 or wider.
A program may use at most 768 MiB of HBM per device.

```python
import jax
import jax.numpy as jnp
from jax import lax

VOCAB_SIZE = 151936
MODEL_DIM = 896
HIDDEN_DIM = 4864
NUM_TOKENS = 512
ROW_BLOCK = 512
NUM_BLOCKS = NUM_TOKENS // ROW_BLOCK
NORM_EPS = 1e-6


def draw_ids(id_key):
    key_base, key_hot, key_pick, key_mix = jax.random.split(id_key, 4)
    base_ids = jax.random.randint(key_base, (NUM_TOKENS,), 0, VOCAB_SIZE, dtype=jnp.int32)
    hot_ids = jax.random.randint(key_hot, (64,), 0, VOCAB_SIZE, dtype=jnp.int32)
    hot_pick = jax.random.randint(key_pick, (NUM_TOKENS,), 0, 64, dtype=jnp.int32)
    use_hot = jax.random.randint(key_mix, (NUM_TOKENS,), 0, 4, dtype=jnp.int32) == 0
    tok_ids = jnp.where(use_hot, hot_ids[hot_pick], base_ids)
    return tok_ids.at[0].set(0).at[NUM_TOKENS - 1].set(VOCAB_SIZE - 1)


def setup_inputs(seed: int = 0, part: int = 0) -> dict:
    root_key = jax.random.key(seed)
    key_table, key_gain, key_in, key_out = jax.random.split(root_key, 4)
    part_key = jax.random.fold_in(jax.random.key(seed + 1), part)
    key_ids, key_grad = jax.random.split(part_key, 2)
    tok_ids = draw_ids(key_ids)
    emb_table = jax.random.normal(key_table, (VOCAB_SIZE, MODEL_DIM), jnp.float32).astype(jnp.bfloat16)
    norm_gain = jax.random.uniform(key_gain, (MODEL_DIM,), jnp.float32, 0.5, 1.5).astype(jnp.bfloat16)
    w_in = (jax.random.normal(key_in, (MODEL_DIM, HIDDEN_DIM), jnp.float32) * MODEL_DIM ** -0.5).astype(jnp.bfloat16)
    w_out = (jax.random.normal(key_out, (HIDDEN_DIM, MODEL_DIM), jnp.float32) * (1.5 * HIDDEN_DIM ** -0.5)).astype(jnp.bfloat16)
    d_out = jax.random.normal(key_grad, (NUM_TOKENS, MODEL_DIM), jnp.float32).astype(jnp.bfloat16)
    return {'tok_ids': tok_ids, 'emb_table': emb_table, 'norm_gain': norm_gain, 'w_in': w_in, 'w_out': w_out, 'd_out': d_out}


def gelu_f32(values):
    return jax.nn.gelu(values, approximate=True)


def reference(tok_ids, emb_table, norm_gain, w_in, w_out, d_out):
    gain_f32 = norm_gain.astype(jnp.float32)
    x_rows = jnp.take(emb_table, tok_ids, axis=0)
    x_blocks = x_rows.reshape(NUM_BLOCKS, ROW_BLOCK, MODEL_DIM)
    grad_blocks = d_out.reshape(NUM_BLOCKS, ROW_BLOCK, MODEL_DIM)

    def body(carry, block):
        acc_in, acc_out = carry
        x_blk, grad_blk = block
        x_f32 = x_blk.astype(jnp.float32)
        inv_rms = lax.rsqrt(jnp.mean(x_f32 * x_f32, axis=-1, keepdims=True) + NORM_EPS)
        x_hat = x_f32 * inv_rms
        normed = (x_hat * gain_f32).astype(jnp.bfloat16)
        pre_act = jnp.dot(normed, w_in, preferred_element_type=jnp.float32).astype(jnp.bfloat16)
        act_f32, gelu_vjp = jax.vjp(gelu_f32, pre_act.astype(jnp.float32))
        hidden = act_f32.astype(jnp.bfloat16)
        mlp_out = jnp.dot(hidden, w_out, preferred_element_type=jnp.float32)
        out_blk = (x_f32 + mlp_out).astype(jnp.bfloat16)
        d_hidden = jnp.dot(grad_blk, w_out.T, preferred_element_type=jnp.float32)
        acc_out = acc_out + jnp.dot(hidden.T, grad_blk, preferred_element_type=jnp.float32)
        d_pre = gelu_vjp(d_hidden)[0].astype(jnp.bfloat16)
        acc_in = acc_in + jnp.dot(normed.T, d_pre, preferred_element_type=jnp.float32)
        d_normed = jnp.dot(d_pre, w_in.T, preferred_element_type=jnp.float32)
        d_hat = d_normed * gain_f32
        d_x = grad_blk.astype(jnp.float32) + inv_rms * (d_hat - x_hat * jnp.mean(d_hat * x_hat, axis=-1, keepdims=True))
        return (acc_in, acc_out), (out_blk, d_x.astype(jnp.bfloat16))

    init = (jnp.zeros((MODEL_DIM, HIDDEN_DIM), jnp.float32), jnp.zeros((HIDDEN_DIM, MODEL_DIM), jnp.float32))
    (d_w_in, d_w_out), (out_blocks, dx_blocks) = lax.scan(body, init, (x_blocks, grad_blocks))
    block_out = out_blocks.reshape(NUM_TOKENS, MODEL_DIM)
    d_x_rows = dx_blocks.reshape(NUM_TOKENS, MODEL_DIM).astype(jnp.float32)
    d_table = jax.ops.segment_sum(d_x_rows, tok_ids, num_segments=VOCAB_SIZE)
    return (block_out, d_table, d_w_in, d_w_out)
```

```python
import functools

import jax
import jax.numpy as jnp
from jax import lax
from jax.experimental import pallas as pl
from jax.experimental.pallas import tpu as pltpu
from jax.sharding import PartitionSpec as P

NORM_EPS = 1e-6
MESH = pl.DeviceIdType.MESH
F32 = jnp.float32
BF16 = jnp.bfloat16
GROUP = 8
LANES = 128


def gather_kernel(n, ids_ref, table_ref, rows_ref, list_ref, count_ref, groups, placed, wide, sem):
    me = lax.axis_index('tp')
    chip, core = me // 2, me % 2
    tokens = ids_ref.shape[0]
    per = tokens // n
    rows_local = table_ref.shape[0]
    base = me * rows_local
    unroll = 16

    def scan(i, count):
        for j in range(unroll):
            token = i * unroll + j
            local = ids_ref[token] - base
            owned = (local >= 0) & (local < rows_local)
            list_ref[count] = local * tokens + token
            count = count + owned.astype(jnp.int32)
        return count

    placed[...] = jnp.zeros_like(placed)
    count = lax.fori_loop(0, tokens // unroll, scan, jnp.int32(0))
    count_ref[0] = count

    def group_copy(k):
        local = list_ref[k] // tokens
        start = pl.multiple_of(local // GROUP * GROUP, GROUP)
        return pltpu.make_async_copy(table_ref.at[pl.ds(start, GROUP)], groups.at[k], sem)

    def fetch(k, _):
        group_copy(k).start()
        return 0

    def settle(k, _):
        group_copy(k).wait()
        return 0

    lax.fori_loop(0, count, fetch, 0)
    lax.fori_loop(0, count, settle, 0)

    def place(k, _):
        entry = list_ref[k]
        token, local = entry % tokens, entry // tokens
        block = token // per
        rel = (block // 2 + n // 2 - chip) % (n // 2) * 2 + (block + core) % 2
        row = rel * per + token % per
        wide[0:GROUP, :] = groups[k].astype(F32)
        placed[pl.ds(row, 1), :] = wide[pl.ds(local % GROUP, 1), :]
        return 0

    lax.fori_loop(0, count, place, 0)
    rows_ref[...] = placed[0:tokens, :].astype(BF16)


def gather_rows(n, tok_ids, table):
    tokens, depth = tok_ids.shape[0], table.shape[1]
    return pl.pallas_call(
        functools.partial(gather_kernel, n),
        out_shape=(
            jax.ShapeDtypeStruct((tokens, depth), BF16),
            jax.ShapeDtypeStruct((tokens + 1,), jnp.int32),
            jax.ShapeDtypeStruct((1,), jnp.int32),
        ),
        in_specs=[pl.BlockSpec(memory_space=pltpu.SMEM), pl.BlockSpec(memory_space=pl.ANY)],
        out_specs=(
            pl.BlockSpec(memory_space=pltpu.VMEM),
            pl.BlockSpec(memory_space=pltpu.SMEM),
            pl.BlockSpec(memory_space=pltpu.SMEM),
        ),
        scratch_shapes=[
            pltpu.VMEM((tokens, GROUP, depth), BF16),
            pltpu.VMEM((tokens + GROUP, depth), F32),
            pltpu.VMEM((2 * GROUP, depth), F32),
            pltpu.SemaphoreType.DMA,
        ],
        compiler_params=pltpu.CompilerParams(vmem_limit_bytes=24 << 20),
        name='gather_rows',
    )(tok_ids, table)


def dot_nt(a, b):
    return lax.dot_general(a, b, (((1,), (1,)), ((), ())), preferred_element_type=F32)


def dot_nn(a, b):
    return lax.dot_general(a, b, (((1,), (0,)), ((), ())), preferred_element_type=F32)


def dot_tn(a, b):
    return lax.dot_general(a, b, (((0,), (0,)), ((), ())), preferred_element_type=F32)


def gelu_and_slope(u):
    c = 0.7978845608028654
    u2 = u * u
    t = jnp.tanh(c * (u + 0.044715 * (u * u2)))
    cdf = 0.5 * (1.0 + t)
    slope = cdf + 0.5 * u * (1.0 - t * t) * (c * (1.0 + 3.0 * 0.044715 * u2))
    return u * cdf, slope


def each(count, step):
    def body(i, carry):
        step(i)
        return carry

    lax.fori_loop(0, count, body, 0)


def block_kernel(n, rows_ref, gain_ref, win_ref, wout_ref, dout_ref,
                 out_ref, nall_ref, gall_ref, hid_ref, dpre_ref, dxall_ref,
                 win, wout, slope_dh, y_part, dn_part,
                 x_rx, x_cs, x_o, x_n,
                 y_rx, y_cs, y_o, y_n,
                 d_rx, d_cs, d_o, d_n,
                 load_sem, send_sem, recv_sem):
    chips = n // 2
    me = lax.axis_index('tp')
    chip, core = me // 2, me % 2
    partner = chip * 2 + (1 - core)
    per = dout_ref.shape[0]
    half = per // 2
    hidden = win_ref.shape[0]
    padded = win.shape[0]

    def side(d):
        return (chip + 1 + 2 * d) % chips * 2 + core

    loads = [
        pltpu.make_async_copy(win_ref, win.at[pl.ds(0, hidden)], load_sem.at[0]),
        pltpu.make_async_copy(wout_ref, wout.at[pl.ds(0, hidden)], load_sem.at[1]),
    ]
    for load in loads:
        load.start()

    barrier = pltpu.get_barrier_semaphore()
    for peer in (partner, side(0), side(1)):
        pl.semaphore_signal(barrier, inc=1, device_id={'tp': peer}, device_id_type=MESH)
    pl.semaphore_wait(barrier, 3)

    groups = []

    class Copies:
        def __init__(self, count, route):
            self.count, self.route = count, route
            self.base = sum(g.count for g in groups)
            groups.append(self)

        def at(self, i):
            src, dst, peer = self.route(i)
            return pltpu.make_async_remote_copy(
                src_ref=src, dst_ref=dst, send_sem=send_sem.at[self.base + i], recv_sem=recv_sem.at[self.base + i],
                device_id={'tp': peer}, device_id_type=MESH)

        def start(self, i):
            self.at(i).start()

        def arrive(self, i):
            self.at(i).wait_recv()

        def start_all(self):
            each(self.count, self.start)

        def arrive_all(self):
            each(self.count, self.arrive)

        def drain(self):
            each(self.count, lambda i: self.at(i).wait_send())

    def tok(q, s):
        return pl.ds(pl.multiple_of((2 * q + s) * per, per), per)

    def tok_half(q, s, h):
        return pl.ds(pl.multiple_of((2 * q + s) * per + h * half, half), half)

    def half_of(h):
        return pl.ds(pl.multiple_of(h * half, half), half)

    def tok_pair(q):
        return pl.ds(pl.multiple_of(2 * q * per, 2 * per), 2 * per)

    class Scatter:
        def __init__(self, part, rx, cs, opp, near):
            self.part, self.rx, self.cs, self.opp, self.lr = part, rx, cs, opp, near
            self.shared = Copies(chips, lambda q: (part.at[tok(q, 1)], rx.at[q], partner))
            self.far = Copies(2, lambda d: (cs.at[2, half_of(d)], opp.at[d], side(d)))
            self.near = Copies(2, lambda d: (cs.at[1 + 2 * d, half_of(1 - d)], near.at[d, half_of(1 - d)], side(d)))
            self.last = Copies(2, lambda d: (cs.at[1 + 2 * d, half_of(d)], near.at[d, half_of(d)], side(d)))

        def share(self, q):
            self.shared.start(q)

        def add(self, q):
            self.shared.arrive(q)
            total = self.part[tok(q, 0), :].astype(F32) + self.rx[q].astype(F32)
            self.cs[q] = total.astype(self.cs.dtype)

        def add_sides(self):
            each(2, lambda d: self.add(1 + 2 * d))

        def forward(self):
            def step(d):
                self.far.arrive(d)
                rows = half_of(d)
                total = self.cs[1 + 2 * d, rows].astype(F32) + self.opp[d].astype(F32)
                self.cs[1 + 2 * d, rows] = total.astype(self.cs.dtype)
                self.last.start(d)

            each(2, step)

        def total(self):
            self.near.arrive_all()
            self.last.arrive_all()
            return self.cs[0].astype(F32) + self.lr[0].astype(F32) + self.lr[1].astype(F32)

    class Gather:
        def __init__(self, own, buf):
            self.pair = Copies(1, lambda i: (own, buf.at[tok(0, 1)], partner))
            self.first = Copies(2, lambda d: (own.at[half_of(d)], buf.at[tok_half(3 - 2 * d, 0, d)], side(d)))
            self.second = Copies(2, lambda d: (own.at[half_of(1 - d)], buf.at[tok_half(3 - 2 * d, 0, 1 - d)], side(d)))
            self.far = Copies(2, lambda d: (buf.at[tok_half(3 - 2 * d, 0, d)], buf.at[tok_half(2, 0, d)], side(d)))
            self.near_pair = Copies(2, lambda d: (buf.at[tok(3 - 2 * d, 0)], buf.at[tok(3 - 2 * d, 1)], partner))
            self.far_pair = Copies(2, lambda d: (buf.at[tok_half(2, 0, d)], buf.at[tok_half(2, 1, d)], partner))

        def begin(self):
            self.first.start_all()
            self.second.start_all()

        def relay(self):
            def step(d):
                self.first.arrive(d)
                self.far.start(d)

            each(2, step)

        def pass_near(self):
            def step(d):
                self.second.arrive(d)
                self.near_pair.start(d)

            each(2, step)

        def pass_far(self):
            def step(d):
                self.far.arrive(d)
                self.far_pair.start(d)

            each(2, step)

    x_sum = Scatter(rows_ref, x_rx, x_cs, x_o, x_n)
    each(chips, lambda i: x_sum.share((i + 2) % chips))
    grads = Gather(dout_ref, gall_ref)
    grads.pair.start(0)
    gall_ref[tok(0, 0), :] = dout_ref[...]
    win[hidden:padded, :] = jnp.zeros((padded - hidden, win.shape[1]), BF16)
    wout[hidden:padded, :] = jnp.zeros((padded - hidden, wout.shape[1]), BF16)
    x_sum.add(2)
    x_sum.far.start_all()
    x_sum.add_sides()
    x_sum.near.start_all()
    x_sum.add(0)
    x_sum.forward()
    grads.begin()
    x_own = x_sum.total()

    gain = gain_ref[...].astype(F32)
    inv_rms = lax.rsqrt(jnp.mean(x_own * x_own, axis=-1, keepdims=True) + NORM_EPS)
    x_hat = x_own * inv_rms
    nall_ref[tok(0, 0), :] = (x_hat * gain).astype(BF16)
    norms = Gather(nall_ref.at[tok(0, 0)], nall_ref)
    norms.begin()
    norms.pair.start(0)

    for load in loads:
        load.wait()

    def back_in(q):
        slope_dh[tok_pair(q), :] = dot_nt(gall_ref[tok_pair(q), :], wout[...])

    def mlp(q):
        rows = tok_pair(q)
        u = dot_nt(nall_ref[rows, :], win[...]).astype(BF16).astype(F32)
        act, slope = gelu_and_slope(u)
        hid_ref[rows, :] = act.astype(BF16)
        d_pre = (slope_dh[rows, :] * slope).astype(BF16)
        dpre_ref[rows, :] = d_pre
        dn_part[rows, :] = dot_nn(d_pre, win[...])

    def mlp_out(q):
        rows = tok_pair(q)
        y_part[rows, :] = dot_nn(hid_ref[rows, :], wout[...])

    dn_sum = Scatter(dn_part, d_rx, d_cs, d_o, d_n)
    y_sum = Scatter(y_part, y_rx, y_cs, y_o, y_n)

    grads.relay()
    grads.pass_near()
    grads.pair.arrive(0)
    back_in(0)
    norms.relay()
    norms.pass_near()
    norms.pair.arrive(0)
    mlp(0)
    dn_sum.share(0)

    def near_in(d):
        grads.near_pair.arrive(d)
        back_in(3 - 2 * d)

    each(2, near_in)
    grads.pass_far()
    norms.pass_far()

    def near_mlp(d):
        norms.near_pair.arrive(d)
        mlp(3 - 2 * d)
        dn_sum.share(3 - 2 * d)

    each(2, near_mlp)
    grads.far_pair.arrive_all()
    back_in(2)
    dn_sum.add_sides()
    dn_sum.near.start_all()
    norms.far_pair.arrive_all()
    mlp(2)
    dn_sum.share(2)

    def near_out(d):
        mlp_out(1 + 2 * d)
        y_sum.share(1 + 2 * d)

    each(1, near_out)
    dn_sum.add(2)
    dn_sum.far.start_all()
    each(1, lambda d: near_out(d + 1))
    dn_sum.add(0)
    y_sum.add_sides()
    y_sum.near.start_all()
    mlp_out(2)
    y_sum.share(2)
    dn_sum.forward()
    y_sum.add(2)
    y_sum.far.start_all()
    mlp_out(0)
    y_sum.share(0)

    d_hat = dn_sum.total() * gain
    d_x = dout_ref[...].astype(F32) + inv_rms * (d_hat - x_hat * jnp.mean(d_hat * x_hat, axis=-1, keepdims=True))
    dxall_ref[tok(0, 0), :] = d_x.astype(BF16)
    grads_x = Gather(dxall_ref.at[tok(0, 0)], dxall_ref)
    grads_x.begin()
    grads_x.pair.start(0)
    y_sum.forward()
    grads_x.relay()
    grads_x.pass_near()
    y_sum.add(0)
    out_ref[...] = (x_own + y_sum.total()).astype(BF16)
    grads_x.pass_far()
    for copies in (grads_x.pair, grads_x.near_pair, grads_x.far_pair):
        copies.arrive_all()
    for copies in groups:
        copies.drain()


def run_block(n, rows, gain, win_t, w_out, d_out):
    tokens, depth = rows.shape
    per = tokens // n
    hidden = win_t.shape[0]
    padded = -(-hidden // LANES) * LANES
    copies = 64
    vm = pl.BlockSpec(memory_space=pltpu.VMEM)
    hbm = pl.BlockSpec(memory_space=pl.ANY)

    def scatter_scratch(dtype):
        return [
            pltpu.VMEM((n // 2, per, depth), dtype),
            pltpu.VMEM((n // 2, per, depth), dtype),
            pltpu.VMEM((2, per // 2, depth), dtype),
            pltpu.VMEM((2, per, depth), dtype),
        ]

    return pl.pallas_call(
        functools.partial(block_kernel, n),
        out_shape=(
            jax.ShapeDtypeStruct((per, depth), BF16),
            jax.ShapeDtypeStruct((tokens, depth), BF16),
            jax.ShapeDtypeStruct((tokens, depth), BF16),
            jax.ShapeDtypeStruct((tokens, padded), BF16),
            jax.ShapeDtypeStruct((tokens, padded), BF16),
            jax.ShapeDtypeStruct((tokens, depth), BF16),
        ),
        in_specs=[vm, vm, hbm, hbm, vm],
        out_specs=(vm,) * 6,
        scratch_shapes=[
            pltpu.VMEM((padded, depth), BF16),
            pltpu.VMEM((padded, depth), BF16),
            pltpu.VMEM((tokens, padded), F32),
            pltpu.VMEM((tokens, depth), F32),
            pltpu.VMEM((tokens, depth), F32),
            *scatter_scratch(BF16),
            *scatter_scratch(F32),
            *scatter_scratch(F32),
            pltpu.SemaphoreType.DMA((2,)),
            pltpu.SemaphoreType.DMA((copies,)),
            pltpu.SemaphoreType.DMA((copies,)),
        ],
        compiler_params=pltpu.CompilerParams(
            collective_id=0, has_side_effects=True, vmem_limit_bytes=40 << 20),
        name='block',
    )(rows, gain, win_t, w_out, d_out)


def table_kernel(n, list_ref, count_ref, bo_ref, nall_ref, gall_ref, hid_ref, dpre_ref, dx_ref,
                 table_ref, dwin_ref, dwout_ref, out_ref,
                 zeros, wide, sums, dwin, dwout, slot_of, group_of, zero_sem, row_sem, w_sem):
    me = lax.axis_index('tp')
    chip, core = me // 2, me % 2
    rows_local, depth = table_ref.shape
    tokens = dx_ref.shape[0]
    per = tokens // n
    chunk = zeros.shape[0]
    fills, rest = rows_local // chunk, rows_local % chunk
    hidden = dwin_ref.shape[0]
    groups = rows_local // GROUP

    def fill(i):
        start = pl.multiple_of(i * chunk, GROUP)
        return pltpu.make_async_copy(zeros, table_ref.at[pl.ds(start, chunk)], zero_sem)

    def fill_rest():
        return pltpu.make_async_copy(
            zeros.at[pl.ds(0, rest)], table_ref.at[pl.ds(fills * chunk, rest)], zero_sem)

    def begin(i, _):
        fill(i).start()
        return 0

    def finish(i, _):
        fill(i).wait()
        return 0

    zeros[...] = jnp.zeros_like(zeros)
    lax.fori_loop(0, fills, begin, 0)
    if rest:
        fill_rest().start()
    out_ref[...] = bo_ref[...]

    w_copies = [
        pltpu.make_async_copy(dwout.at[pl.ds(0, hidden)], dwout_ref, w_sem.at[0]),
        pltpu.make_async_copy(dwin.at[pl.ds(0, hidden)], dwin_ref, w_sem.at[1]),
    ]
    for j in range(0, dwout.shape[0], LANES):
        dwout[j:j + LANES, :] = dot_tn(hid_ref[:, j:j + LANES], gall_ref[...])
    w_copies[0].start()
    for j in range(0, dwin.shape[0], LANES):
        dwin[j:j + LANES, :] = dot_tn(dpre_ref[:, j:j + LANES], nall_ref[...])
    w_copies[1].start()

    wide[0:tokens, :] = dx_ref[...].astype(F32)
    unroll = 2

    def clear(i, _):
        for j in range(unroll):
            slot_of[i * unroll + j] = -1
        return 0

    lax.fori_loop(0, groups // unroll, clear, 0)
    count = count_ref[0]

    def gather_up(k, slots):
        entry = list_ref[k]
        token, local = entry % tokens, entry // tokens
        block = token // per
        rel = (block // 2 + n // 2 - chip) % (n // 2) * 2 + (block + core) % 2
        row = rel * per + token % per
        group = local // GROUP
        known = slot_of[group]
        fresh = known < 0
        slot = jnp.where(fresh, slots, known)
        slot_of[group] = slot
        group_of[slot] = group
        sub = lax.broadcasted_iota(jnp.int32, (GROUP, depth), 0)
        line = jnp.broadcast_to(wide[pl.ds(row, 1), :], (GROUP, depth))
        before = jnp.where(fresh, 0.0, sums[slot])
        sums[slot] = before + jnp.where(sub == local % GROUP, line, 0.0)
        return slots + fresh.astype(jnp.int32)

    slots = lax.fori_loop(0, count, gather_up, jnp.int32(0))
    lax.fori_loop(0, fills, finish, 0)
    if rest:
        fill_rest().wait()

    def write(k):
        start = pl.multiple_of(group_of[k] * GROUP, GROUP)
        return pltpu.make_async_copy(sums.at[k], table_ref.at[pl.ds(start, GROUP)], row_sem)

    def put(k, _):
        write(k).start()
        return 0

    def done(k, _):
        write(k).wait()
        return 0

    lax.fori_loop(0, slots, put, 0)
    lax.fori_loop(0, slots, done, 0)
    for copy in w_copies:
        copy.wait()


def finish_grads(n, rows_local, hidden, owned, count, block_out, n_all, g_all, hid, d_pre, dx_all):
    tokens, depth = dx_all.shape
    padded = hid.shape[1]
    vm = pl.BlockSpec(memory_space=pltpu.VMEM)
    sm = pl.BlockSpec(memory_space=pltpu.SMEM)
    hbm = pl.BlockSpec(memory_space=pl.ANY)
    return pl.pallas_call(
        functools.partial(table_kernel, n),
        out_shape=(
            jax.ShapeDtypeStruct((rows_local, depth), F32),
            jax.ShapeDtypeStruct((hidden, depth), F32),
            jax.ShapeDtypeStruct((hidden, depth), F32),
            jax.ShapeDtypeStruct(block_out.shape, BF16),
        ),
        in_specs=[sm, sm, vm, vm, vm, vm, vm, vm],
        out_specs=(hbm, hbm, hbm, vm),
        scratch_shapes=[
            pltpu.VMEM((592, depth), F32),
            pltpu.VMEM((tokens + GROUP, depth), F32),
            pltpu.VMEM((tokens, GROUP, depth), F32),
            pltpu.VMEM((padded, depth), F32),
            pltpu.VMEM((padded, depth), F32),
            pltpu.SMEM((rows_local // GROUP,), jnp.int32),
            pltpu.SMEM((tokens,), jnp.int32),
            pltpu.SemaphoreType.DMA,
            pltpu.SemaphoreType.DMA,
            pltpu.SemaphoreType.DMA((2,)),
        ],
        compiler_params=pltpu.CompilerParams(vmem_limit_bytes=40 << 20),
        name='table_grad',
    )(owned, count, block_out, n_all, g_all, hid, d_pre, dx_all)


def solution(mesh):
    n = mesh.shape['tp']

    def device_step(tok_ids, emb_shard, norm_gain, w_in, w_out, d_out):
        rows, owned, count = gather_rows(n, tok_ids, emb_shard)
        block_out, n_all, g_all, hid, d_pre, dx_all = run_block(
            n, rows, norm_gain.reshape(1, -1), w_in.T, w_out, d_out)
        d_table, d_win_t, d_w_out, block_out = finish_grads(
            n, emb_shard.shape[0], w_out.shape[0], owned, count, block_out, n_all, g_all, hid, d_pre, dx_all)
        return block_out, d_table, d_win_t.T, d_w_out

    return jax.shard_map(
        device_step,
        mesh=mesh,
        in_specs=(P('dp'), P('tp', None), P(None), P(None, 'tp'), P('tp', None), P(('dp', 'tp'), None)),
        out_specs=(P(('dp', 'tp'), None), P(('dp', 'tp'), None), P('dp', 'tp'), P(('dp', 'tp'), None)),
        check_vma=False,
    )
```

```python
import functools

import jax
import jax.numpy as jnp
from jax import lax
from jax.experimental import pallas as pl
from jax.experimental.pallas import tpu as pltpu
from jax.sharding import PartitionSpec as P

NORM_EPS = 1e-6
MESH = pl.DeviceIdType.MESH
F32 = jnp.float32
BF16 = jnp.bfloat16
GROUP = 8
LANES = 128
CHUNK = 592
FILL_GATHER, FILL_OUT = 9, 16


def each(count, step):
    def body(i, carry):
        step(i)
        return carry

    lax.fori_loop(0, count, body, 0)


class Fill:
    def __init__(self, zeros, table_ref, sem, first, last):
        self.zeros, self.table, self.sem, self.first, self.last = zeros, table_ref, sem, first, last
        self.chunk = zeros.shape[0]
        self.rows = table_ref.shape[0]

    def at(self, i):
        start = pl.multiple_of((self.first + i) * self.chunk, GROUP)
        return pltpu.make_async_copy(self.zeros, self.table.at[pl.ds(start, self.chunk)], self.sem)

    def rest(self):
        full = self.rows // self.chunk
        tail = self.rows - full * self.chunk
        if self.last < full or not tail:
            return None
        return pltpu.make_async_copy(
            self.zeros.at[pl.ds(0, tail)], self.table.at[pl.ds(full * self.chunk, tail)], self.sem)

    def start(self):
        self.zeros[...] = jnp.zeros_like(self.zeros)
        each(self.last - self.first, lambda i: self.at(i).start())
        rest = self.rest()
        if rest:
            rest.start()

    def wait(self):
        each(self.last - self.first, lambda i: self.at(i).wait())
        rest = self.rest()
        if rest:
            rest.wait()


def chunks_of(rows, part):
    return rows // CHUNK * part // 32


def gather_kernel(n, ids_hbm, table_ref, rows_ref, list_ref, count_ref, dtable_ref,
                  ids_ref, groups, placed, wide, zeros, sem, ids_sem, fill_sem):
    load_ids = pltpu.make_async_copy(ids_hbm, ids_ref, ids_sem)
    load_ids.start()
    me = lax.axis_index('tp')
    chip, core = me // 2, me % 2
    tokens = ids_ref.shape[0]
    per = tokens // n
    rows_local = table_ref.shape[0]
    base = me * rows_local
    unroll = 16
    fill = Fill(zeros, dtable_ref, fill_sem, 0, chunks_of(rows_local, FILL_GATHER))
    fill.start()

    def scan(i, count):
        for j in range(unroll):
            token = i * unroll + j
            local = ids_ref[token] - base
            owned = (local >= 0) & (local < rows_local)
            list_ref[count] = local * tokens + token
            count = count + owned.astype(jnp.int32)
        return count

    placed[...] = jnp.zeros_like(placed)
    load_ids.wait()
    count = lax.fori_loop(0, tokens // unroll, scan, jnp.int32(0))
    count_ref[0] = count

    def group_copy(k):
        local = list_ref[k] // tokens
        start = pl.multiple_of(local // GROUP * GROUP, GROUP)
        return pltpu.make_async_copy(table_ref.at[pl.ds(start, GROUP)], groups.at[k], sem)

    each(count, lambda k: group_copy(k).start())
    each(count, lambda k: group_copy(k).wait())

    def place(k):
        entry = list_ref[k]
        token, local = entry % tokens, entry // tokens
        block = token // per
        rel = (block // 2 + n // 2 - chip) % (n // 2) * 2 + (block + core) % 2
        row = rel * per + token % per
        wide[0:GROUP, :] = groups[k].astype(F32)
        placed[pl.ds(row, 1), :] = wide[pl.ds(local % GROUP, 1), :]

    each(count, place)
    rows_ref[...] = placed[0:tokens, :].astype(BF16)
    fill.wait()


def gather_rows(n, tok_ids, table):
    tokens, depth = tok_ids.shape[0], table.shape[1]
    hbm = pl.BlockSpec(memory_space=pl.ANY)
    return pl.pallas_call(
        functools.partial(gather_kernel, n),
        out_shape=(
            jax.ShapeDtypeStruct((tokens, depth), BF16),
            jax.ShapeDtypeStruct((tokens + 1,), jnp.int32),
            jax.ShapeDtypeStruct((1,), jnp.int32),
            jax.ShapeDtypeStruct(table.shape, F32),
        ),
        in_specs=[pl.BlockSpec(memory_space=pltpu.HBM), hbm],
        out_specs=(
            pl.BlockSpec(memory_space=pltpu.VMEM),
            pl.BlockSpec(memory_space=pltpu.SMEM),
            pl.BlockSpec(memory_space=pltpu.SMEM),
            hbm,
        ),
        scratch_shapes=[
            pltpu.SMEM((tokens,), jnp.int32),
            pltpu.VMEM((tokens, GROUP, depth), BF16),
            pltpu.VMEM((tokens + GROUP, depth), F32),
            pltpu.VMEM((2 * GROUP, depth), F32),
            pltpu.VMEM((CHUNK, depth), F32),
            pltpu.SemaphoreType.DMA,
            pltpu.SemaphoreType.DMA,
            pltpu.SemaphoreType.DMA,
        ],
        compiler_params=pltpu.CompilerParams(vmem_limit_bytes=24 << 20),
        name='gather_rows',
    )(tok_ids, table)


def dot_nt(a, b):
    return lax.dot_general(a, b, (((1,), (1,)), ((), ())), preferred_element_type=F32)


def dot_nn(a, b):
    return lax.dot_general(a, b, (((1,), (0,)), ((), ())), preferred_element_type=F32)


def dot_tn(a, b):
    return lax.dot_general(a, b, (((0,), (0,)), ((), ())), preferred_element_type=F32)


def gelu_and_slope(u):
    c = 0.7978845608028654
    u2 = u * u
    t = jnp.tanh(c * (u + 0.044715 * (u * u2)))
    cdf = 0.5 * (1.0 + t)
    slope = cdf + 0.5 * u * (1.0 - t * t) * (c * (1.0 + 3.0 * 0.044715 * u2))
    return u * cdf, slope


def block_kernel(n, rows_ref, gain_ref, win_ref, wout_ref, dout_ref,
                 out_ref, nall_ref, gall_ref, hid_ref, dpre_ref, dx_ref,
                 win, wout, slope_dh, y_part, dn_part,
                 x_rx, x_cs, x_o, x_n,
                 y_rx, y_cs, y_o, y_n,
                 d_rx, d_cs, d_o, d_n,
                 load_sem, send_sem, recv_sem):
    chips = n // 2
    me = lax.axis_index('tp')
    chip, core = me // 2, me % 2
    partner = chip * 2 + (1 - core)
    per = dout_ref.shape[0]
    half = per // 2
    hidden = win_ref.shape[0]
    padded = win.shape[0]

    def side(d):
        return (chip + 1 + 2 * d) % chips * 2 + core

    loads = [
        pltpu.make_async_copy(win_ref, win.at[pl.ds(0, hidden)], load_sem.at[0]),
        pltpu.make_async_copy(wout_ref, wout.at[pl.ds(0, hidden)], load_sem.at[1]),
    ]
    for load in loads:
        load.start()

    barrier = pltpu.get_barrier_semaphore()
    for peer in (partner, side(0), side(1)):
        pl.semaphore_signal(barrier, inc=1, device_id={'tp': peer}, device_id_type=MESH)
    pl.semaphore_wait(barrier, 3)

    groups = []

    class Copies:
        def __init__(self, count, route):
            self.count, self.route = count, route
            self.base = sum(g.count for g in groups)
            groups.append(self)

        def at(self, i):
            src, dst, peer = self.route(i)
            return pltpu.make_async_remote_copy(
                src_ref=src, dst_ref=dst, send_sem=send_sem.at[self.base + i], recv_sem=recv_sem.at[self.base + i],
                device_id={'tp': peer}, device_id_type=MESH)

        def start(self, i):
            self.at(i).start()

        def arrive(self, i):
            self.at(i).wait_recv()

        def start_all(self):
            each(self.count, self.start)

        def arrive_all(self):
            each(self.count, self.arrive)

        def drain(self):
            each(self.count, lambda i: self.at(i).wait_send())

    def tok(q, s):
        return pl.ds(pl.multiple_of((2 * q + s) * per, per), per)

    def tok_half(q, s, h):
        return pl.ds(pl.multiple_of((2 * q + s) * per + h * half, half), half)

    def half_of(h):
        return pl.ds(pl.multiple_of(h * half, half), half)

    def tok_pair(q):
        return pl.ds(pl.multiple_of(2 * q * per, 2 * per), 2 * per)

    class Scatter:
        def __init__(self, part, rx, cs, opp, near):
            self.part, self.rx, self.cs, self.opp, self.lr = part, rx, cs, opp, near
            self.shared = Copies(chips, lambda q: (part.at[tok(q, 1)], rx.at[q], partner))
            self.far = Copies(2, lambda d: (cs.at[2, half_of(d)], opp.at[d], side(d)))
            self.near = Copies(2, lambda d: (cs.at[1 + 2 * d, half_of(1 - d)], near.at[d, half_of(1 - d)], side(d)))
            self.last = Copies(2, lambda d: (cs.at[1 + 2 * d, half_of(d)], near.at[d, half_of(d)], side(d)))

        def share(self, q):
            self.shared.start(q)

        def add(self, q):
            self.shared.arrive(q)
            total = self.part[tok(q, 0), :].astype(F32) + self.rx[q].astype(F32)
            self.cs[q] = total.astype(self.cs.dtype)

        def add_sides(self):
            each(2, lambda d: self.add(1 + 2 * d))

        def forward(self):
            def step(d):
                self.far.arrive(d)
                rows = half_of(d)
                total = self.cs[1 + 2 * d, rows].astype(F32) + self.opp[d].astype(F32)
                self.cs[1 + 2 * d, rows] = total.astype(self.cs.dtype)
                self.last.start(d)

            each(2, step)

        def total(self):
            self.near.arrive_all()
            self.last.arrive_all()
            return self.cs[0].astype(F32) + self.lr[0].astype(F32) + self.lr[1].astype(F32)

    class Gather:
        def __init__(self, own, buf):
            self.pair = Copies(1, lambda i: (own, buf.at[tok(0, 1)], partner))
            self.first = Copies(2, lambda d: (own.at[half_of(d)], buf.at[tok_half(3 - 2 * d, 0, d)], side(d)))
            self.second = Copies(2, lambda d: (own.at[half_of(1 - d)], buf.at[tok_half(3 - 2 * d, 0, 1 - d)], side(d)))
            self.far = Copies(2, lambda d: (buf.at[tok_half(3 - 2 * d, 0, d)], buf.at[tok_half(2, 0, d)], side(d)))
            self.near_pair = Copies(2, lambda d: (buf.at[tok(3 - 2 * d, 0)], buf.at[tok(3 - 2 * d, 1)], partner))
            self.far_pair = Copies(2, lambda d: (buf.at[tok_half(2, 0, d)], buf.at[tok_half(2, 1, d)], partner))

        def begin(self):
            self.first.start_all()
            self.second.start_all()

        def relay(self):
            def step(d):
                self.first.arrive(d)
                self.far.start(d)

            each(2, step)

        def pass_near(self):
            def step(d):
                self.second.arrive(d)
                self.near_pair.start(d)

            each(2, step)

        def pass_far(self):
            def step(d):
                self.far.arrive(d)
                self.far_pair.start(d)

            each(2, step)

    x_sum = Scatter(rows_ref, x_rx, x_cs, x_o, x_n)
    each(chips, lambda i: x_sum.share((i + 2) % chips))
    grads = Gather(dout_ref, gall_ref)
    grads.pair.start(0)
    gall_ref[tok(0, 0), :] = dout_ref[...]
    win[hidden:padded, :] = jnp.zeros((padded - hidden, win.shape[1]), BF16)
    wout[hidden:padded, :] = jnp.zeros((padded - hidden, wout.shape[1]), BF16)
    x_sum.add(2)
    x_sum.far.start_all()
    x_sum.add_sides()
    x_sum.near.start_all()
    x_sum.add(0)
    x_sum.forward()
    grads.begin()
    x_own = x_sum.total()

    gain = gain_ref[...].astype(F32)[None, :]
    inv_rms = lax.rsqrt(jnp.mean(x_own * x_own, axis=-1, keepdims=True) + NORM_EPS)
    x_hat = x_own * inv_rms
    nall_ref[tok(0, 0), :] = (x_hat * gain).astype(BF16)
    norms = Gather(nall_ref.at[tok(0, 0)], nall_ref)
    norms.begin()
    norms.pair.start(0)

    for load in loads:
        load.wait()

    def back_in(q):
        slope_dh[tok_pair(q), :] = dot_nt(gall_ref[tok_pair(q), :], wout[...])

    def mlp(q):
        rows = tok_pair(q)
        u = dot_nt(nall_ref[rows, :], win[...]).astype(BF16).astype(F32)
        act, slope = gelu_and_slope(u)
        hid_ref[rows, :] = act.astype(BF16)
        d_pre = (slope_dh[rows, :] * slope).astype(BF16)
        dpre_ref[rows, :] = d_pre
        dn_part[rows, :] = dot_nn(d_pre, win[...])

    def mlp_out(q):
        rows = tok_pair(q)
        y_part[rows, :] = dot_nn(hid_ref[rows, :], wout[...])

    dn_sum = Scatter(dn_part, d_rx, d_cs, d_o, d_n)
    y_sum = Scatter(y_part, y_rx, y_cs, y_o, y_n)

    grads.relay()
    grads.pass_near()
    grads.pair.arrive(0)
    back_in(0)
    norms.relay()
    norms.pass_near()
    norms.pair.arrive(0)
    mlp(0)
    dn_sum.share(0)

    def near_in(d):
        grads.near_pair.arrive(d)
        back_in(3 - 2 * d)

    each(2, near_in)
    grads.pass_far()
    norms.pass_far()

    def near_mlp(d):
        norms.near_pair.arrive(d)
        mlp(3 - 2 * d)
        dn_sum.share(3 - 2 * d)

    each(2, near_mlp)
    grads.far_pair.arrive_all()
    back_in(2)
    dn_sum.add_sides()
    dn_sum.near.start_all()
    norms.far_pair.arrive_all()
    mlp(2)
    dn_sum.share(2)

    def near_out(d):
        mlp_out(1 + 2 * d)
        y_sum.share(1 + 2 * d)

    each(1, near_out)
    dn_sum.add(2)
    dn_sum.far.start_all()
    each(1, lambda d: near_out(d + 1))
    dn_sum.add(0)
    y_sum.add_sides()
    y_sum.near.start_all()
    mlp_out(2)
    y_sum.share(2)
    dn_sum.forward()
    y_sum.add(2)
    y_sum.far.start_all()
    mlp_out(0)
    y_sum.share(0)

    d_hat = dn_sum.total() * gain
    d_x = dout_ref[...].astype(F32) + inv_rms * (d_hat - x_hat * jnp.mean(d_hat * x_hat, axis=-1, keepdims=True))
    dx_ref[...] = d_x.astype(BF16)
    y_sum.add(0)
    y_sum.forward()
    out_ref[...] = (x_own + y_sum.total()).astype(BF16)
    for copies in groups:
        copies.drain()


def run_block(n, rows, gain, win_t, w_out, d_out):
    tokens, depth = rows.shape
    per = tokens // n
    hidden = win_t.shape[0]
    padded = -(-hidden // LANES) * LANES
    copies = 64
    vm = pl.BlockSpec(memory_space=pltpu.VMEM)
    hbm = pl.BlockSpec(memory_space=pl.ANY)

    def scatter_scratch(dtype):
        return [
            pltpu.VMEM((n // 2, per, depth), dtype),
            pltpu.VMEM((n // 2, per, depth), dtype),
            pltpu.VMEM((2, per // 2, depth), dtype),
            pltpu.VMEM((2, per, depth), dtype),
        ]

    return pl.pallas_call(
        functools.partial(block_kernel, n),
        out_shape=(
            jax.ShapeDtypeStruct((per, depth), BF16),
            jax.ShapeDtypeStruct((tokens, depth), BF16),
            jax.ShapeDtypeStruct((tokens, depth), BF16),
            jax.ShapeDtypeStruct((tokens, padded), BF16),
            jax.ShapeDtypeStruct((tokens, padded), BF16),
            jax.ShapeDtypeStruct((per, depth), BF16),
        ),
        in_specs=[vm, vm, hbm, hbm, vm],
        out_specs=(vm,) * 6,
        scratch_shapes=[
            pltpu.VMEM((padded, depth), BF16),
            pltpu.VMEM((padded, depth), BF16),
            pltpu.VMEM((tokens, padded), F32),
            pltpu.VMEM((tokens, depth), F32),
            pltpu.VMEM((tokens, depth), F32),
            *scatter_scratch(BF16),
            *scatter_scratch(F32),
            *scatter_scratch(F32),
            pltpu.SemaphoreType.DMA((2,)),
            pltpu.SemaphoreType.DMA((copies,)),
            pltpu.SemaphoreType.DMA((copies,)),
        ],
        compiler_params=pltpu.CompilerParams(
            collective_id=0, has_side_effects=True, vmem_limit_bytes=40 << 20),
        name='block',
    )(rows, gain, win_t, w_out, d_out)


def weight_out_kernel(hid_ref, gall_ref, table_in, table_ref, dw_ref, dw, zeros, fill_sem, w_sem):
    rows_local = table_ref.shape[0]
    fill = Fill(zeros, table_ref, fill_sem,
                chunks_of(rows_local, FILL_GATHER), chunks_of(rows_local, FILL_GATHER + FILL_OUT))
    fill.start()
    for j in range(0, dw.shape[0], LANES):
        dw[j:j + LANES, :] = dot_tn(hid_ref[:, j:j + LANES], gall_ref[...])
    copy = pltpu.make_async_copy(dw.at[pl.ds(0, dw_ref.shape[0])], dw_ref, w_sem)
    copy.start()
    copy.wait()
    fill.wait()


def weight_in_kernel(n, list_ref, count_ref, bo_ref, dpre_ref, nall_ref, table_in, table_ref, dw_ref, out_ref,
                     plan_ref, group_ref, counts_ref, dw, zeros, slot_of, fill_sem, w_sem):
    me = lax.axis_index('tp')
    chip, core = me // 2, me % 2
    rows_local = table_ref.shape[0]
    tokens = nall_ref.shape[0]
    per = tokens // n
    groups = rows_local // GROUP
    fill = Fill(zeros, table_ref, fill_sem,
                chunks_of(rows_local, FILL_GATHER + FILL_OUT), chunks_of(rows_local, 32))
    fill.start()
    out_ref[...] = bo_ref[...]
    for j in range(0, dw.shape[0], LANES):
        dw[j:j + LANES, :] = dot_tn(dpre_ref[:, j:j + LANES], nall_ref[...])
    copy = pltpu.make_async_copy(dw.at[pl.ds(0, dw_ref.shape[0])], dw_ref, w_sem)
    copy.start()
    unroll = 2

    def clear(i):
        for j in range(unroll):
            slot_of[i * unroll + j] = -1

    each(groups // unroll, clear)
    count = count_ref[0]

    def plan(k, slots):
        entry = list_ref[k]
        token, local = entry % tokens, entry // tokens
        block = token // per
        rel = (block // 2 + n // 2 - chip) % (n // 2) * 2 + (block + core) % 2
        row = rel * per + token % per
        group = local // GROUP
        known = slot_of[group]
        fresh = (known < 0).astype(jnp.int32)
        slot = jnp.where(known < 0, slots, known)
        slot_of[group] = slot
        group_ref[slot] = group
        plan_ref[k] = ((fresh * tokens + slot) * tokens + row) * GROUP + local % GROUP
        return slots + fresh

    counts_ref[0] = count
    counts_ref[1] = lax.fori_loop(0, count, plan, jnp.int32(0))
    copy.wait()
    fill.wait()


def table_kernel(n, plan_ref, group_ref, counts_ref, *refs):
    blocks, (table_in, table_ref, wide, sums, row_sem) = refs[:n], refs[n:]
    per, depth = blocks[0].shape
    tokens = n * per
    for i, block in enumerate(blocks):
        wide[i * per:(i + 1) * per, :] = block[...].astype(F32)

    def gather_up(k):
        entry = plan_ref[k]
        sub, entry = entry % GROUP, entry // GROUP
        row, entry = entry % tokens, entry // tokens
        slot, fresh = entry % tokens, entry // tokens
        index = lax.broadcasted_iota(jnp.int32, (GROUP, depth), 0)
        line = jnp.broadcast_to(wide[pl.ds(row, 1), :], (GROUP, depth))
        before = jnp.where(fresh > 0, 0.0, sums[slot])
        sums[slot] = before + jnp.where(index == sub, line, 0.0)

    each(counts_ref[0], gather_up)

    def write(k):
        start = pl.multiple_of(group_ref[k] * GROUP, GROUP)
        return pltpu.make_async_copy(sums.at[k], table_ref.at[pl.ds(start, GROUP)], row_sem)

    slots = counts_ref[1]
    each(slots, lambda k: write(k).start())
    each(slots, lambda k: write(k).wait())


VM = pl.BlockSpec(memory_space=pltpu.VMEM)
SM = pl.BlockSpec(memory_space=pltpu.SMEM)
HBM = pl.BlockSpec(memory_space=pl.ANY)


def weight_out(hid, g_all, d_table, hidden):
    rows_local, depth = d_table.shape
    padded = hid.shape[1]
    return pl.pallas_call(
        weight_out_kernel,
        out_shape=(jax.ShapeDtypeStruct(d_table.shape, F32), jax.ShapeDtypeStruct((hidden, depth), F32)),
        in_specs=[VM, VM, HBM],
        out_specs=(HBM, HBM),
        input_output_aliases={2: 0},
        scratch_shapes=[
            pltpu.VMEM((padded, depth), F32),
            pltpu.VMEM((CHUNK, depth), F32),
            pltpu.SemaphoreType.DMA,
            pltpu.SemaphoreType.DMA,
        ],
        compiler_params=pltpu.CompilerParams(vmem_limit_bytes=16 << 20),
        cost_estimate=pl.CostEstimate(flops=4 * 10**9, bytes_accessed=36 << 20, transcendentals=0),
        name='weight_out',
    )(hid, g_all, d_table)


def weight_in(n, owned, count, block_out, d_pre, n_all, d_table, hidden):
    rows_local, depth = d_table.shape
    tokens, padded = d_pre.shape
    return pl.pallas_call(
        functools.partial(weight_in_kernel, n),
        out_shape=(
            jax.ShapeDtypeStruct(d_table.shape, F32),
            jax.ShapeDtypeStruct((hidden, depth), F32),
            jax.ShapeDtypeStruct(block_out.shape, BF16),
            jax.ShapeDtypeStruct((tokens,), jnp.int32),
            jax.ShapeDtypeStruct((tokens,), jnp.int32),
            jax.ShapeDtypeStruct((2,), jnp.int32),
        ),
        in_specs=[SM, SM, VM, VM, VM, HBM],
        out_specs=(HBM, HBM, VM, SM, SM, SM),
        input_output_aliases={5: 0},
        scratch_shapes=[
            pltpu.VMEM((padded, depth), F32),
            pltpu.VMEM((CHUNK, depth), F32),
            pltpu.SMEM((rows_local // GROUP,), jnp.int32),
            pltpu.SemaphoreType.DMA,
            pltpu.SemaphoreType.DMA,
        ],
        compiler_params=pltpu.CompilerParams(vmem_limit_bytes=16 << 20),
        cost_estimate=pl.CostEstimate(flops=2 * 10**9, bytes_accessed=16 << 20, transcendentals=0),
        name='weight_in',
    )(owned, count, block_out, d_pre, n_all, d_table)


def write_rows(n, plan, groups, counts, blocks, d_table):
    tokens, depth = plan.shape[0], d_table.shape[1]
    return pl.pallas_call(
        functools.partial(table_kernel, n),
        out_shape=jax.ShapeDtypeStruct(d_table.shape, F32),
        in_specs=[SM, SM, SM] + [VM] * n + [HBM],
        out_specs=HBM,
        input_output_aliases={3 + n: 0},
        scratch_shapes=[
            pltpu.VMEM((tokens + GROUP, depth), F32),
            pltpu.VMEM((tokens, GROUP, depth), F32),
            pltpu.SemaphoreType.DMA,
        ],
        compiler_params=pltpu.CompilerParams(vmem_limit_bytes=24 << 20),
        name='table_grad',
    )(plan, groups, counts, *blocks, d_table)


def solution(mesh):
    n = mesh.shape['tp']
    chips = n // 2

    def shifted(block, q, s):
        pairs = []
        for d in range(n):
            source = (d // 2 + q) % chips * 2 + (d + s) % 2
            pairs.append((source, d))
        return lax.ppermute(block, 'tp', pairs)

    def device_step(tok_ids, emb_shard, norm_gain, w_in, w_out, d_out):
        hidden = w_out.shape[0]
        rows, owned, count, d_table = gather_rows(n, tok_ids, emb_shard)
        block_out, n_all, g_all, hid, d_pre, d_x = run_block(n, rows, norm_gain, w_in.T, w_out, d_out)
        own = [d_x] + [shifted(d_x, q, 0) for q in range(1, chips)]
        other = [shifted(block, 0, 1) for block in own]
        d_table, d_w_out = weight_out(hid, g_all, d_table, hidden)
        d_table, d_win_t, block_out, plan, groups, counts = weight_in(
            n, owned, count, block_out, d_pre, n_all, d_table, hidden)
        blocks = [block for pair in zip(own, other) for block in pair]
        d_table = write_rows(n, plan, groups, counts, blocks, d_table)
        return block_out, d_table, d_win_t.T, d_w_out

    return jax.shard_map(
        device_step,
        mesh=mesh,
        in_specs=(P('dp'), P('tp', None), P(None), P(None, 'tp'), P('tp', None), P(('dp', 'tp'), None)),
        out_specs=(P(('dp', 'tp'), None), P(('dp', 'tp'), None), P('dp', 'tp'), P(('dp', 'tp'), None)),
        check_vma=False,
    )
```
